256 devices in a mesh: orb: 16 (over y, x_lo, core), walk: 16 (over z, x_hi).
Axes of the slice: x: 4 (x_hi: 2, x_lo: 2; x = x_hi * 2 + x_lo), y: 4, z: 8, core: 2. Of those that a mesh axis runs over, the one named last changes fastest.
Arguments:
- chol: bfloat16 [64, 2048, 2048], P(None, 'orb', 'walk'), may hold values from -6 to 6
- orbitals: bfloat16 [2048, 1024], replicated, may hold values from -0.125 to 0.125
- greens: bfloat16 [16, 1024, 2048], P('walk'), may hold values from -0.00390625 to 0.00390625
- shift: float32 [64], P('orb'), may hold values from -6 to 6
Outputs:
- force_bias: float32 [16, 64], P('walk', 'orb')
- rotated: bfloat16 [64, 1024, 2048], P('orb', None, 'walk')
The draws below stay inside these ranges and needn't reach their ends.
All inputs are finite; a program needn't handle non-finite values.
Results may differ from the reference program's by a relative error of at most 0.007.
Values may be sent and summed in bfloat16 or wider, within the bound.
A program may use at most 64 MiB of HBM per device.

```python
import jax
import jax.numpy as jnp
from jax import lax

N = 2048
NOCC = 1024
NV = 64
W = 16


def shard_levels(stream_key, shape, pieces, smallest, top_value):
    def one(dim, parts):
        heights = jax.random.uniform(jax.random.fold_in(jax.random.fold_in(stream_key, 6), dim), (parts,), jnp.float32, smallest / len(pieces), top_value / len(pieces))
        return jnp.repeat(jnp.exp(heights), shape[dim] // parts).reshape((-1,) + (1,) * (len(shape) - dim - 1))

    factor_of = one(*pieces[0])
    for cut in pieces[1:]:
        factor_of = factor_of * one(*cut)
    return factor_of


def normal_values(own_key, shape, width, limit, split=(), kind=jnp.bfloat16):
    loudness = shard_levels(own_key, shape, split, -0.22, 0.18) if split else 1.0
    result = jax.random.normal(own_key, shape, jnp.float32) * width * loudness
    return jnp.minimum(jnp.maximum(result, -limit), limit).astype(kind)


def setup_inputs(seed: int = 0) -> dict:
    key_list = jax.random.split(jax.random.key(seed), 5)
    chol = normal_values(key_list[0], (NV, N, N), 1.0, 6.0, ((1, 16), (2, 16)))
    orbitals = normal_values(key_list[1], (N, NOCC), N ** -0.5, 0.125)
    greens = normal_values(key_list[2], (W, NOCC, N), (NOCC * N) ** -0.5, 0.00390625, ((0, 16),))
    shift = normal_values(key_list[3], (NV,), 1.0, 6.0, ((0, 16),), jnp.float32)
    return dict(chol=chol, orbitals=orbitals, greens=greens, shift=shift)


def reference(chol, orbitals, greens, shift):
    flat_greens = greens.reshape(greens.shape[0], -1).astype(jnp.float32)
    orbitals_t = orbitals.T

    def one_vector(matrix):
        rotation = jnp.dot(orbitals_t, matrix, preferred_element_type=jnp.float32)
        column = jnp.dot(flat_greens, rotation.reshape(-1), precision=lax.Precision.HIGHEST)
        return rotation.astype(jnp.bfloat16), column

    rotated, columns = lax.map(one_vector, chol)
    force_bias = columns.T - shift[None, :]
    return (force_bias, rotated)
```

```python
import jax
import jax.numpy as jnp
from jax import lax
from jax.experimental import pallas as pl
from jax.experimental.pallas import tpu as pltpu
from jax.sharding import PartitionSpec as P

MESH = pl.DeviceIdType.MESH
F32, BF16 = jnp.float32, jnp.bfloat16
FAR_FIRST = (4, 3, 5, 2, 6, 1, 7, 0)
CHIPS = ((0, 0), (1, 0), (3, 0), (2, 0), (2, 1), (1, 1), (3, 1), (0, 1))


def kernel(
    chol, orbitals, greens, shift, fb_out, rot_out,
    rows_v, greens_v, orb_v, orb_t, chol_v, chunks, acc,
    t_out, t_in, diag, part_out, part_in, sum_out, sum_in,
    orb_ready, walk_ready, load_sem, greens_sem,
    chol_send, chol_recv, t_send, t_recv, part_send, part_recv, sum_send, sum_recv,
):
    o, w = lax.axis_index("orb"), lax.axis_index("walk")
    y, a, c = o // 4, (o // 2) % 2, o % 2
    z, h = w // 2, w % 2
    across = y * 4 + (1 - a) * 2 + c
    pair = (o // 2) * 2
    partner = pair + 1 - c

    def place(orb, walk):
        return {"orb": orb, "walk": walk}

    def met(walk):
        return place(jnp.where(walk % 2 == h, o, across), walk)

    def signal(sem, where):
        pl.semaphore_signal(sem, inc=1, device_id=where, device_id_type=MESH)

    def await_some(sem, amount):
        @pl.when(amount > 0)
        def _():
            pl.semaphore_wait(sem, amount)

    def loop(start, stop, body):
        lax.fori_loop(start, stop, lambda i, _: body(i), None)

    barrier = pltpu.get_barrier_semaphore()
    signal(barrier, place(partner, w))
    loop(pair + 2, 16, lambda i: signal(barrier, place(i, w)))
    loop(w + 1, 16, lambda i: signal(barrier, met(i)))

    own_rows = pltpu.make_async_copy(
        orbitals.at[pl.ds(pl.multiple_of(o * 128, 128), 128)], rows_v.at[h], load_sem.at[0]
    )
    far_rows = pltpu.make_async_copy(
        orbitals.at[pl.ds(pl.multiple_of(across * 128, 128), 128)], rows_v.at[1 - h], load_sem.at[1]
    )
    own_rows.start()
    far_rows.start()
    columns = []
    for k, dz in enumerate(FAR_FIRST):
        there = pl.multiple_of(((z + dz) % 8) * 256, 256)
        copy = pltpu.make_async_copy(
            greens.at[0, :, pl.ds(there, 256)], greens_v.at[k], greens_sem.at[k]
        )
        copy.start()
        columns.append(copy)
    all_rows = pltpu.make_async_copy(orbitals, orb_v, load_sem.at[2])
    all_rows.start()
    own_chol = pltpu.make_async_copy(chol, chol_v, load_sem.at[3])
    own_chol.start()
    own_chunk = pltpu.make_async_copy(chol.at[pl.ds(4 * o, 4)], chunks.at[o], load_sem.at[4])
    own_chunk.start()

    pl.semaphore_wait(barrier, pair + 1 + w)
    loop(0, pair, lambda i: signal(orb_ready, place(i, w)))
    loop(0, w, lambda i: signal(walk_ready, met(i)))

    def chunk_copy(to):
        return pltpu.make_async_remote_copy(
            src_ref=chol.at[pl.ds(4 * to, 4)],
            dst_ref=chunks.at[o],
            send_sem=chol_send.at[to],
            recv_sem=chol_recv.at[o],
            device_id=place(to, w),
            device_id_type=MESH,
        )

    def chunk_arrival(source):
        pltpu.make_async_remote_copy(
            src_ref=chol.at[pl.ds(4 * source, 4)],
            dst_ref=chunks.at[source],
            send_sem=chol_send.at[source],
            recv_sem=chol_recv.at[source],
            device_id=place(source, w),
            device_id_type=MESH,
        ).wait_recv()

    def chip(dy, da):
        return ((y + dy) % 4) * 2 + (a + da) % 2

    await_some(orb_ready, 14 - pair)
    for dy, da in ((2, 1), (1, 1), (3, 1), (0, 1), (2, 0), (1, 0), (3, 0)):
        for dc in range(2):
            chunk_copy(chip(dy, da) * 2 + (c + dc) % 2).start()
    chunk_copy(partner).start()

    own_rows.wait()
    far_rows.wait()
    for k, dz in enumerate(FAR_FIRST):
        columns[k].wait()
        there = (z + dz) % 8
        both = jnp.dot(
            rows_v[...].reshape(256, 1024), greens_v[k], preferred_element_type=F32
        ).astype(BF16)
        t_out[2 * there] = both[:128, :128]
        t_out[2 * there + 1] = both[128:, 128:]

    def t_copy(to, source):
        return pltpu.make_async_remote_copy(
            src_ref=t_out.at[to],
            dst_ref=t_in.at[source],
            send_sem=t_send.at[to],
            recv_sem=t_recv.at[source],
            device_id=met(to),
            device_id_type=MESH,
        )

    await_some(walk_ready, 15 - w)
    for dz in FAR_FIRST:
        for dh in (1, 0):
            if dz or dh:
                t_copy(((z + dz) % 8) * 2 + (h + dh) % 2, w).start()
    t_in[w] = t_out[w]

    all_rows.wait()

    def turn(i):
        at = pl.ds(pl.multiple_of(i * 128, 128), 128)
        orb_t[:, at] = orb_v[at, :].T

    loop(0, 16, turn)

    def rotate(which):
        dy, da = CHIPS[which]
        there = chip(dy, da)
        if which == 0:
            own_chunk.wait()
            chunk_arrival(partner)
        else:
            chunk_arrival(2 * there)
            chunk_arrival(2 * there + 1)
        block = jnp.concatenate(
            [
                jnp.concatenate([chunks[2 * there, g], chunks[2 * there + 1, g]], axis=0)
                for g in range(4)
            ],
            axis=1,
        )
        at = pl.ds(pl.multiple_of(there * 256, 256), 256)

        def rows(i):
            here = pl.ds(pl.multiple_of(i * 256, 256), 256)
            term = jnp.dot(orb_t[here, at], block, preferred_element_type=F32)
            if which:
                term = acc[here, :] + term
            if which < 7:
                acc[here, :] = term
            else:
                for g in range(4):
                    rot_out[g, here, :] = term[:, g * 128 : (g + 1) * 128].astype(BF16)

        loop(0, 4, rows)

    lane = lax.broadcasted_iota(jnp.int32, (256, 128), 1)
    row = lax.broadcasted_iota(jnp.int32, (256, 128), 0)
    same_row = (lane % 16) == (row % 16)

    def part_copy(to, source):
        return pltpu.make_async_remote_copy(
            src_ref=part_out.at[to],
            dst_ref=part_in.at[source],
            send_sem=part_send.at[to],
            recv_sem=part_recv.at[source],
            device_id=met(to),
            device_id_type=MESH,
        )

    def terms(first):
        for k in range(first, first + 8):
            @pl.when(w != k)
            def _():
                t_copy(k, k).wait_recv()

        right = jnp.concatenate(
            [t_in[first : first + 8, 16 * b : 16 * b + 16, :].reshape(128, 128) for b in range(8)],
            axis=1,
        )

        def vectors(j):
            at = pl.ds(pl.multiple_of(j * 16, 16), 16)
            left = jnp.concatenate(
                [chol_v[at, 16 * b : 16 * b + 16, :].reshape(256, 128) for b in range(8)],
                axis=1,
            )
            product = lax.dot_general(
                left, right, (((1,), (1,)), ((), ())), preferred_element_type=F32
            )
            kept = jnp.where(same_row, product, 0.0)
            diag[at, :] = kept.reshape(16, 16, 128).sum(axis=1)

        loop(0, 4, vectors)
        picks = jnp.where(
            lax.broadcasted_iota(jnp.int32, (8, 128), 1) // 16
            == lax.broadcasted_iota(jnp.int32, (8, 128), 0),
            1.0, 0.0,
        )
        sums = lax.dot_general(
            picks, diag[...], (((1,), (1,)), ((), ())),
            precision=lax.Precision.HIGHEST, preferred_element_type=F32,
        )
        for k in range(8):
            part_out[first + k] = jnp.broadcast_to(sums[k : k + 1, :], (8, 128))
        for k in range(first, first + 8):
            @pl.when(w != k)
            def _():
                part_copy(k, w).start()

    diag[64:, :] = jnp.zeros((64, 128), F32)
    for which in range(4):
        rotate(which)
    own_chol.wait()
    terms(0)
    rotate(4)
    terms(8)
    rotate(5)
    rotate(6)

    part_in[w] = part_out[w]
    for k in range(16):
        @pl.when(w != k)
        def _():
            part_copy(k, k).wait_recv()

    sum_out[...] = part_in[...].sum(axis=0)

    def sum_copy(to, source):
        return pltpu.make_async_remote_copy(
            src_ref=sum_out,
            dst_ref=sum_in.at[source],
            send_sem=sum_send.at[to],
            recv_sem=sum_recv.at[source],
            device_id=place(to, w),
            device_id_type=MESH,
        )

    for k in range(16):
        @pl.when(o != k)
        def _():
            sum_copy(k, o).start()
    sum_in[o] = sum_out[...]
    rotate(7)
    for k in range(16):
        @pl.when(o != k)
        def _():
            sum_copy(k, k).wait_recv()

    total = pltpu.roll(sum_in[...].sum(axis=0), (128 - 4 * o) % 128, 1)[:1]
    spot = lax.broadcasted_iota(jnp.int32, (1, 128), 1)
    moved = jnp.zeros((1, 128), F32)
    for j in range(4):
        moved = jnp.where(spot == j, shift[j], moved)
    fb_out[...] = (total - moved)[:, :4]

    for k in range(16):
        @pl.when(o != k)
        def _():
            chunk_copy(k).wait_send()
            sum_copy(k, o).wait_send()

        @pl.when(w != k)
        def _():
            t_copy(k, w).wait_send()
            part_copy(k, w).wait_send()


def local(chol, orbitals, greens, shift):
    anywhere = pl.BlockSpec(memory_space=pl.ANY)
    in_vmem = pl.BlockSpec(memory_space=pltpu.VMEM)
    sems = [pltpu.SemaphoreType.DMA((16,))] * 8
    return pl.pallas_call(
        kernel,
        out_shape=(
            jax.ShapeDtypeStruct((1, 4), F32),
            jax.ShapeDtypeStruct((4, 1024, 128), BF16),
        ),
        in_specs=[anywhere, anywhere, anywhere, pl.BlockSpec(memory_space=pltpu.SMEM)],
        out_specs=(in_vmem, in_vmem),
        scratch_shapes=[
            pltpu.VMEM((2, 128, 1024), BF16),
            pltpu.VMEM((8, 1024, 256), BF16),
            pltpu.VMEM((2048, 1024), BF16),
            pltpu.VMEM((1024, 2048), BF16),
            pltpu.VMEM((64, 128, 128), BF16),
            pltpu.VMEM((16, 4, 128, 128), BF16),
            pltpu.VMEM((1024, 512), F32),
            pltpu.VMEM((16, 128, 128), BF16),
            pltpu.VMEM((16, 128, 128), BF16),
            pltpu.VMEM((128, 128), F32),
            pltpu.VMEM((16, 8, 128), F32),
            pltpu.VMEM((16, 8, 128), F32),
            pltpu.VMEM((8, 128), F32),
            pltpu.VMEM((16, 8, 128), F32),
            pltpu.SemaphoreType.REGULAR,
            pltpu.SemaphoreType.REGULAR,
            pltpu.SemaphoreType.DMA((5,)),
            pltpu.SemaphoreType.DMA((8,)),
            *sems,
        ],
        compiler_params=pltpu.CompilerParams(
            collective_id=0, has_side_effects=True, vmem_limit_bytes=62 * 2**20
        ),
        name="half_rotation",
    )(chol, orbitals, greens, shift)


def solution(mesh):
    return jax.shard_map(
        local,
        mesh=mesh,
        in_specs=(P(None, "orb", "walk"), P(), P("walk", None, None), P("orb")),
        out_specs=(P("walk", "orb"), P("orb", None, "walk")),
        check_vma=False,
    )
```

```python
import jax
import jax.numpy as jnp
from jax import lax
from jax.experimental import pallas as pl
from jax.experimental.pallas import tpu as pltpu
from jax.sharding import PartitionSpec as P

MESH = pl.DeviceIdType.MESH
F32, BF16 = jnp.float32, jnp.bfloat16
FAR_FIRST = (4, 3, 5, 2, 6, 1, 7, 0)

def kernel(
    chol, orbitals, greens, fb_out, rot_out,
    rows_v, greens_v, orb_v, orb_t, chol_v, chunks, acc,
    t_out, t_in, diag, part_out, part_in, sum_out, sum_in,
    orb_ready, walk_ready, load_sem, greens_sem,
    chol_send, chol_recv, t_send, t_recv, part_send, part_recv, sum_send, sum_recv,
):
    o, w = lax.axis_index("orb"), lax.axis_index("walk")
    y, a, c = o // 4, (o // 2) % 2, o % 2
    z, h = w // 2, w % 2
    across = y * 4 + (1 - a) * 2 + c
    pair = (o // 2) * 2
    partner = pair + 1 - c

    def place(orb, walk):
        return {"orb": orb, "walk": walk}

    def met(walk):
        return place(jnp.where(walk % 2 == h, o, across), walk)

    def signal(sem, where):
        pl.semaphore_signal(sem, inc=1, device_id=where, device_id_type=MESH)

    def await_some(sem, amount):
        @pl.when(amount > 0)
        def _():
            pl.semaphore_wait(sem, amount)

    def loop(start, stop, body):
        lax.fori_loop(start, stop, lambda i, _: body(i), None)

    es = jax.named_scope('e_sig'); es.__enter__()
    barrier = pltpu.get_barrier_semaphore()
    signal(barrier, place(partner, w))
    loop(pair + 2, 16, lambda i: signal(barrier, place(i, w)))
    loop(w + 1, 16, lambda i: signal(barrier, met(i)))

    es.__exit__(None,None,None)
    es = jax.named_scope('e_load'); es.__enter__()
    own_rows = pltpu.make_async_copy(
        orbitals.at[pl.ds(pl.multiple_of(o * 128, 128), 128)], rows_v.at[h], load_sem.at[0]
    )
    far_rows = pltpu.make_async_copy(
        orbitals.at[pl.ds(pl.multiple_of(across * 128, 128), 128)], rows_v.at[1 - h], load_sem.at[1]
    )
    own_rows.start()
    far_rows.start()
    columns = []
    for k, dz in enumerate(FAR_FIRST):
        there = pl.multiple_of(((z + dz) % 8) * 256, 256)
        copy = pltpu.make_async_copy(
            greens.at[0, :, pl.ds(there, 256)], greens_v.at[k], greens_sem.at[k]
        )
        copy.start()
        columns.append(copy)
    all_rows = pltpu.make_async_copy(orbitals, orb_v, load_sem.at[2])
    all_rows.start()
    own_chol = pltpu.make_async_copy(chol, chol_v, load_sem.at[3])
    own_chol.start()
    own_chunk = pltpu.make_async_copy(chol.at[pl.ds(4 * o, 4)], chunks.at[o], load_sem.at[4])
    own_chunk.start()

    es.__exit__(None,None,None)
    with jax.named_scope("w_bar"):
        pl.semaphore_wait(barrier, pair + 1 + w)
    loop(0, w, lambda i: signal(walk_ready.at[w // 8], met(i)))
    loop(0, pair, lambda i: signal(orb_ready, place(i, w)))

    def chunk_copy(to):
        return pltpu.make_async_remote_copy(
            src_ref=chol.at[pl.ds(4 * to, 4)],
            dst_ref=chunks.at[o],
            send_sem=chol_send.at[to],
            recv_sem=chol_recv.at[o],
            device_id=place(to, w),
            device_id_type=MESH,
        )

    def chunk_arrival(source):
        pltpu.make_async_remote_copy(
            src_ref=chol.at[pl.ds(4 * source, 4)],
            dst_ref=chunks.at[source],
            send_sem=chol_send.at[source],
            recv_sem=chol_recv.at[source],
            device_id=place(source, w),
            device_id_type=MESH,
        ).wait_recv()

    def chip(dy, da):
        return ((y + dy) % 4) * 2 + (a + da) % 2

    order = ((2, 1), (1, 1), (3, 1), (0, 1), (2, 0), (1, 0), (3, 0))

    def scatter_all():
        with jax.named_scope("w_orb"):
            await_some(orb_ready, 14 - pair)
        for dy, da in order:
            for dc in range(2):
                chunk_copy(chip(dy, da) * 2 + (c + dc) % 2).start()
        chunk_copy(partner).start()

    def products():
        own_rows.wait()
        far_rows.wait()
        for k, dz in enumerate(FAR_FIRST):
            columns[k].wait()
            there = (z + dz) % 8
            both = jnp.dot(
                rows_v[...].reshape(256, 1024), greens_v[k], preferred_element_type=F32
            ).astype(BF16)
            t_out[2 * there] = both[:128, :128]
            t_out[2 * there + 1] = both[128:, 128:]

    @pl.when(y < 2)
    def _():
        with jax.named_scope("prod"):
            products()
        scatter_all()

    @pl.when(y >= 2)
    def _():
        scatter_all()
        with jax.named_scope("prod"):
            products()

    def t_copy(to, source):
        return pltpu.make_async_remote_copy(
            src_ref=t_out.at[to],
            dst_ref=t_in.at[source],
            send_sem=t_send.at[to],
            recv_sem=t_recv.at[source],
            device_id=met(to),
            device_id_type=MESH,
        )

    def send_products(wanted):
        for dz in FAR_FIRST:
            for dh in (1, 0):
                to = ((z + dz) % 8) * 2 + (h + dh) % 2

                @pl.when(wanted(to))
                def _():
                    t_copy(to, w).start()

    with jax.named_scope("w_walk0"):
        await_some(walk_ready.at[0], 7 - w)
    send_products(lambda to: (to < 8) & (to != w))
    with jax.named_scope("w_walk1"):
        await_some(walk_ready.at[1], jnp.where(w < 8, 8, 15 - w))
    send_products(lambda to: (to >= 8) & (to != w))
    t_in[w] = t_out[w]

    all_rows.wait()

    def turn(i):
        at = pl.ds(pl.multiple_of(i * 128, 128), 128)
        orb_t[:, at] = orb_v[at, :].T

    with jax.named_scope("turn"):
        loop(0, 16, turn)

    def rotate(group, first=False, last=False):
        spots = []
        for dy, da in group:
            there = chip(dy, da)
            with jax.named_scope(f"w_c{dy}{da}"):
                if dy or da:
                    chunk_arrival(2 * there)
                    chunk_arrival(2 * there + 1)
                else:
                    own_chunk.wait()
                    chunk_arrival(partner)
            spots.append(there)
        with jax.named_scope(f"rot{group[0][0]}{group[0][1]}"):
            left = jnp.concatenate(
                [orb_t[:, pl.ds(pl.multiple_of(there * 256, 256), 256)] for there in spots], axis=1
            )
            for n in range(2):
                block = jnp.concatenate(
                    [
                        jnp.concatenate(
                            [chunks[2 * there + i, g] for there in spots for i in range(2)], axis=0
                        )
                        for g in (2 * n, 2 * n + 1)
                    ],
                    axis=1,
                )
                term = jnp.dot(left, block, preferred_element_type=F32)
                at = slice(256 * n, 256 * n + 256)
                if not first:
                    term = acc[:, at] + term
                if last:
                    rot_out[2 * n] = term[:, :128].astype(BF16)
                    rot_out[2 * n + 1] = term[:, 128:].astype(BF16)
                else:
                    acc[:, at] = term

    lane = lax.broadcasted_iota(jnp.int32, (256, 128), 1)
    row = lax.broadcasted_iota(jnp.int32, (256, 128), 0)
    same_row = (lane % 16) == (row % 16)

    def part_copy(to, source):
        return pltpu.make_async_remote_copy(
            src_ref=part_out.at[to],
            dst_ref=part_in.at[source],
            send_sem=part_send.at[to],
            recv_sem=part_recv.at[source],
            device_id=met(to),
            device_id_type=MESH,
        )

    def terms(first):
        with jax.named_scope(f"w_t{first}"):
          for k in range(first, first + 8):
            @pl.when(w != k)
            def _():
                t_copy(k, k).wait_recv()
        tsc = jax.named_scope(f"terms{first}"); tsc.__enter__()

        right = jnp.concatenate(
            [t_in[first : first + 8, 16 * b : 16 * b + 16, :].reshape(128, 128) for b in range(8)],
            axis=1,
        )

        for j in range(4):
            at = slice(16 * j, 16 * j + 16)
            left = jnp.concatenate(
                [chol_v[at, 16 * b : 16 * b + 16, :].reshape(256, 128) for b in range(8)],
                axis=1,
            )
            product = lax.dot_general(
                left, right, (((1,), (1,)), ((), ())), preferred_element_type=F32
            )
            kept = jnp.where(same_row, product, 0.0)
            diag[at, :] = kept.reshape(16, 16, 128).sum(axis=1)

        picks = jnp.where(
            lax.broadcasted_iota(jnp.int32, (8, 128), 1) // 16
            == lax.broadcasted_iota(jnp.int32, (8, 128), 0),
            1.0, 0.0,
        )
        sums = lax.dot_general(
            picks, diag[...], (((1,), (1,)), ((), ())),
            precision=lax.Precision.HIGHEST, preferred_element_type=F32,
        )
        for k in range(8):
            part_out[first + k] = jnp.broadcast_to(sums[k : k + 1, :], (8, 128))
        for k in range(first, first + 8):
            @pl.when(w != k)
            def _():
                part_copy(k, w).start()
        tsc.__exit__(None,None,None)

    diag[64:, :] = jnp.zeros((64, 128), F32)
    rotate(((0, 0),), first=True)
    own_chol.wait()
    terms(0)
    terms(8)
    rotate(((2, 0), (2, 1)))
    rotate(((1, 1), (3, 1)))
    part_in[w] = part_out[w]
    with jax.named_scope("w_part"):
      for k in range(16):
        @pl.when(w != k)
        def _():
            part_copy(k, k).wait_recv()

    sum_out[...] = part_in[...].sum(axis=0)

    def sum_copy(to, source):
        return pltpu.make_async_remote_copy(
            src_ref=sum_out,
            dst_ref=sum_in.at[source],
            send_sem=sum_send.at[to],
            recv_sem=sum_recv.at[source],
            device_id=place(to, w),
            device_id_type=MESH,
        )

    for k in range(16):
        @pl.when(o != k)
        def _():
            sum_copy(k, o).start()
    sum_in[o] = sum_out[...]
    rotate(((1, 0), (3, 0), (0, 1)), last=True)
    with jax.named_scope("w_sum"):
      for k in range(16):
        @pl.when(o != k)
        def _():
            sum_copy(k, k).wait_recv()

    total = pltpu.roll(sum_in[...].sum(axis=0), (128 - 4 * o) % 128, 1)[:1]
    fb_out[...] = total[:, :4]

    with jax.named_scope("w_send"):
      for k in range(16):
        @pl.when(o != k)
        def _():
            chunk_copy(k).wait_send()
            sum_copy(k, o).wait_send()

        @pl.when(w != k)
        def _():
            t_copy(k, w).wait_send()
            part_copy(k, w).wait_send()


def local(chol, orbitals, greens, shift):
    anywhere = pl.BlockSpec(memory_space=pltpu.HBM)
    in_vmem = pl.BlockSpec(memory_space=pltpu.VMEM)
    sems = [pltpu.SemaphoreType.DMA((16,))] * 8
    force_bias, rotated = pl.pallas_call(
        kernel,
        out_shape=(
            jax.ShapeDtypeStruct((1, 4), F32),
            jax.ShapeDtypeStruct((4, 1024, 128), BF16),
        ),
        in_specs=[anywhere] * 3,
        out_specs=(in_vmem, in_vmem),
        scratch_shapes=[
            pltpu.VMEM((2, 128, 1024), BF16),
            pltpu.VMEM((8, 1024, 256), BF16),
            pltpu.VMEM((2048, 1024), BF16),
            pltpu.VMEM((1024, 2048), BF16),
            pltpu.VMEM((64, 128, 128), BF16),
            pltpu.VMEM((16, 4, 128, 128), BF16),
            pltpu.VMEM((1024, 512), F32),
            pltpu.VMEM((16, 128, 128), BF16),
            pltpu.VMEM((16, 128, 128), BF16),
            pltpu.VMEM((128, 128), F32),
            pltpu.VMEM((16, 8, 128), F32),
            pltpu.VMEM((16, 8, 128), F32),
            pltpu.VMEM((8, 128), F32),
            pltpu.VMEM((16, 8, 128), F32),
            pltpu.SemaphoreType.REGULAR,
            pltpu.SemaphoreType.REGULAR((2,)),
            pltpu.SemaphoreType.DMA((5,)),
            pltpu.SemaphoreType.DMA((8,)),
            *sems,
        ],
        compiler_params=pltpu.CompilerParams(
            collective_id=0, has_side_effects=True, vmem_limit_bytes=52 * 2**20
        ),
        name="half_rotation",
    )(chol, orbitals, greens)
    return force_bias - shift[None, :], rotated


def solution(mesh):
    return jax.shard_map(
        local,
        mesh=mesh,
        in_specs=(P(None, "orb", "walk"), P(), P("walk", None, None), P("orb")),
        out_specs=(P("walk", "orb"), P("orb", None, "walk")),
        check_vma=False,
    )
```

```python
import jax
import jax.numpy as jnp
from jax import lax
from jax.experimental import pallas as pl
from jax.experimental.pallas import tpu as pltpu
from jax.sharding import PartitionSpec as P

MESH = pl.DeviceIdType.MESH
F32, BF16 = jnp.float32, jnp.bfloat16
FAR_FIRST = (4, 3, 5, 2, 6, 1, 7, 0)

def kernel(
    chol, orbitals, greens, fb_out, rot_out,
    rows_v, greens_v, orb_v, orb_t, chol_v, chunks, acc,
    t_out, t_in, diag_few, diag_all, part_out, part_in, sum_out, sum_in,
    orb_ready, walk_ready, load_sem, greens_sem,
    chol_send, chol_recv, t_send, t_recv, part_send, part_recv, sum_send, sum_recv,
):
    o, w = lax.axis_index("orb"), lax.axis_index("walk")
    y, a, c = o // 4, (o // 2) % 2, o % 2
    z, h = w // 2, w % 2
    across = y * 4 + (1 - a) * 2 + c
    pair = (o // 2) * 2
    partner = pair + 1 - c

    def place(orb, walk):
        return {"orb": orb, "walk": walk}

    def met(walk):
        return place(jnp.where(walk % 2 == h, o, across), walk)

    def signal(sem, where):
        pl.semaphore_signal(sem, inc=1, device_id=where, device_id_type=MESH)

    def await_some(sem, amount):
        @pl.when(amount > 0)
        def _():
            pl.semaphore_wait(sem, amount)

    def loop(start, stop, body):
        lax.fori_loop(start, stop, lambda i, _: body(i), None)

    es = jax.named_scope('e_sig'); es.__enter__()
    barrier = pltpu.get_barrier_semaphore()
    loop(8, jnp.where(z < 4, 16, 0), lambda i: signal(barrier, met(i)))
    signal(barrier, place(partner, w))
    loop(pair + 2, 16, lambda i: signal(barrier, place(i, w)))
    loop(w + 1, 8, lambda i: signal(barrier, met(i)))

    es.__exit__(None,None,None)
    es = jax.named_scope('e_load'); es.__enter__()
    own_rows = pltpu.make_async_copy(
        orbitals.at[pl.ds(pl.multiple_of(o * 128, 128), 128)], rows_v.at[h], load_sem.at[0]
    )
    far_rows = pltpu.make_async_copy(
        orbitals.at[pl.ds(pl.multiple_of(across * 128, 128), 128)], rows_v.at[1 - h], load_sem.at[1]
    )
    own_rows.start()
    far_rows.start()
    columns = []
    for k, dz in enumerate(FAR_FIRST):
        there = pl.multiple_of(((z + dz) % 8) * 256, 256)
        copy = pltpu.make_async_copy(
            greens.at[0, :, pl.ds(there, 256)], greens_v.at[k], greens_sem.at[k]
        )
        copy.start()
        columns.append(copy)
    es.__exit__(None,None,None)
    with jax.named_scope("w_bar"):
        pl.semaphore_wait(barrier, pair + 1 + jnp.minimum(w, 8))
    loop(0, jnp.minimum(w, 8), lambda i: signal(walk_ready.at[w // 8], met(i)))
    loop(0, pair, lambda i: signal(orb_ready, place(i, w)))

    def chunk_copy(to):
        return pltpu.make_async_remote_copy(
            src_ref=chol.at[pl.ds(4 * to, 4)],
            dst_ref=chunks.at[o],
            send_sem=chol_send.at[to],
            recv_sem=chol_recv.at[o],
            device_id=place(to, w),
            device_id_type=MESH,
        )

    def chunk_arrival(source):
        pltpu.make_async_remote_copy(
            src_ref=chol.at[pl.ds(4 * source, 4)],
            dst_ref=chunks.at[source],
            send_sem=chol_send.at[source],
            recv_sem=chol_recv.at[source],
            device_id=place(source, w),
            device_id_type=MESH,
        ).wait_recv()

    def chip(dy, da):
        return ((y + dy) % 4) * 2 + (a + da) % 2

    order = ((2, 1), (1, 1), (3, 1), (0, 1), (2, 0), (1, 0), (3, 0))

    def scatter_all():
        with jax.named_scope("w_orb"):
            await_some(orb_ready, 14 - pair)
        for dy, da in order:
            for dc in range(2):
                chunk_copy(chip(dy, da) * 2 + (c + dc) % 2).start()
        chunk_copy(partner).start()

    all_rows = pltpu.make_async_copy(orbitals, orb_v, load_sem.at[2])
    own_chol = pltpu.make_async_copy(chol, chol_v, load_sem.at[3])
    own_chunk = pltpu.make_async_copy(chol.at[pl.ds(4 * o, 4)], chunks.at[o], load_sem.at[4])

    def t_copy(to, source):
        return pltpu.make_async_remote_copy(
            src_ref=t_out.at[to],
            dst_ref=t_in.at[source],
            send_sem=t_send.at[to],
            recv_sem=t_recv.at[source],
            device_id=met(to),
            device_id_type=MESH,
        )

    def send_products(wanted):
        for dz in FAR_FIRST:
            for dh in (1, 0):
                to = ((z + dz) % 8) * 2 + (h + dh) % 2

                @pl.when(wanted(to))
                def _():
                    t_copy(to, w).start()

    own_rows.wait()
    far_rows.wait()

    def products(start, stop):
        for k in range(start, stop):
            columns[k].wait()
        for k in range(start, stop):
            there = (z + FAR_FIRST[k]) % 8
            both = jnp.dot(
                rows_v[...].reshape(256, 1024), greens_v[k], preferred_element_type=F32
            ).astype(BF16)
            t_out[2 * there] = both[:128, :128]
            t_out[2 * there + 1] = both[128:, 128:]

    def all_products():
        with jax.named_scope("prod1"):
            products(0, 4)
        all_rows.start()
        own_chol.start()
        own_chunk.start()
        with jax.named_scope("prod"):
            products(4, 8)

        @pl.when(z >= 4)
        def _():
            send_products(lambda to: to < 8)

    @pl.when(y < 2)
    def _():
        all_products()
        scatter_all()

    @pl.when(y >= 2)
    def _():
        scatter_all()
        all_products()

    def products_from(first, count):
        for k in range(first, first + count):

            @pl.when(w != k)
            def _():
                t_copy(k, k).wait_recv()

    patient = (z == 2) | (z == 3)
    with jax.named_scope("w_walk0"):
        await_some(walk_ready.at[0], 7 - w)

    @pl.when(z < 4)
    def _():
        send_products(lambda to: (to < 8) & (to != w))


    all_rows.wait()

    def turn(i):
        at = pl.ds(pl.multiple_of(i * 128, 128), 128)
        orb_t[:, at] = orb_v[at, :].T

    with jax.named_scope("turn"):
        loop(0, 16, turn)

    @pl.when(patient)
    def _():
        with jax.named_scope("w_pat"):
            products_from(0, 2)

    with jax.named_scope("w_walk1"):
        @pl.when(z < 4)
        def _():
            pl.semaphore_wait(walk_ready.at[1], 8)

        @pl.when(w == 7)
        def _():
            loop(8, 16, lambda i: signal(walk_ready.at[0], met(i)))

        @pl.when(z >= 4)
        def _():
            pl.semaphore_wait(walk_ready.at[0], 1)

    send_products(lambda to: (to >= 8) & (to != w))
    t_in[w] = t_out[w]

    def rotate(group, first=False, last=False):
        spots = []
        for dy, da in group:
            there = chip(dy, da)
            with jax.named_scope(f"w_c{dy}{da}"):
                if dy or da:
                    chunk_arrival(2 * there)
                    chunk_arrival(2 * there + 1)
                else:
                    own_chunk.wait()
                    chunk_arrival(partner)
            spots.append(there)
        with jax.named_scope(f"rot{group[0][0]}{group[0][1]}"):
            left = jnp.concatenate(
                [orb_t[:, pl.ds(pl.multiple_of(there * 256, 256), 256)] for there in spots], axis=1
            )
            for n in range(2):
                block = jnp.concatenate(
                    [
                        jnp.concatenate(
                            [chunks[2 * there + i, g] for there in spots for i in range(2)], axis=0
                        )
                        for g in (2 * n, 2 * n + 1)
                    ],
                    axis=1,
                )
                term = jnp.dot(left, block, preferred_element_type=F32)
                at = slice(256 * n, 256 * n + 256)
                if not first:
                    term = acc[:, at] + term
                if last:
                    rot_out[2 * n] = term[:, :128].astype(BF16)
                    rot_out[2 * n + 1] = term[:, 128:].astype(BF16)
                else:
                    acc[:, at] = term

    def part_copy(to, source):
        return pltpu.make_async_remote_copy(
            src_ref=part_out.at[to],
            dst_ref=part_in.at[source],
            send_sem=part_send.at[to],
            recv_sem=part_recv.at[source],
            device_id=met(to),
            device_id_type=MESH,
        )

    def terms(count, skipped, diag):
        lanes = 16 * count
        right = jnp.concatenate(
            [t_in[:count, 16 * b : 16 * b + 16, :].reshape(lanes, 128) for b in range(8)], axis=1
        )
        same_row = (
            lax.broadcasted_iota(jnp.int32, (256, lanes), 1) % 16
            == lax.broadcasted_iota(jnp.int32, (256, lanes), 0) % 16
        )
        for j in range(4):
            at = slice(16 * j, 16 * j + 16)
            left = jnp.concatenate(
                [chol_v[at, 16 * b : 16 * b + 16, :].reshape(256, 128) for b in range(8)],
                axis=1,
            )
            product = lax.dot_general(
                left, right, (((1,), (1,)), ((), ())), preferred_element_type=F32
            )
            diag[at, :] = jnp.where(same_row, product, 0.0).reshape(16, 16, lanes).sum(axis=1)

        picks = jnp.where(
            lax.broadcasted_iota(jnp.int32, (16, lanes), 1) // 16
            == lax.broadcasted_iota(jnp.int32, (16, lanes), 0),
            1.0, 0.0,
        )
        sums = lax.dot_general(
            picks, diag[...], (((1,), (1,)), ((), ())),
            precision=lax.Precision.HIGHEST, preferred_element_type=F32,
        )
        for k in range(skipped, count):
            part_out[k] = jnp.broadcast_to(sums[k : k + 1, :], (8, 128))
        for k in range(skipped, count):

            @pl.when(w != k)
            def _():
                part_copy(k, w).start()

    diag_few[64:, :] = jnp.zeros((64, 64), F32)
    diag_all[64:, :] = jnp.zeros((64, 256), F32)
    rotate(((0, 0),), first=True)
    own_chol.wait()
    with jax.named_scope("w_t0"):

        @pl.when(jnp.logical_not(patient))
        def _():
            products_from(0, 2)

        products_from(2, 2)

    with jax.named_scope("terms0"):
        terms(4, 0, diag_few)
    with jax.named_scope("w_t4"):
        products_from(4, 12)
    with jax.named_scope("terms4"):
        terms(16, 4, diag_all)
    part_in[w] = part_out[w]
    with jax.named_scope("w_part"):
      for k in range(16):
        @pl.when(w != k)
        def _():
            part_copy(k, k).wait_recv()

    sum_out[...] = part_in[...].sum(axis=0)

    def sum_copy(to, source):
        return pltpu.make_async_remote_copy(
            src_ref=sum_out,
            dst_ref=sum_in.at[source],
            send_sem=sum_send.at[to],
            recv_sem=sum_recv.at[source],
            device_id=place(to, w),
            device_id_type=MESH,
        )

    for k in range(16):
        @pl.when(o != k)
        def _():
            sum_copy(k, o).start()
    sum_in[o] = sum_out[...]
    rotate(((2, 0), (2, 1)))
    rotate(((1, 1), (3, 1)))
    rotate(((1, 0), (3, 0), (0, 1)), last=True)
    with jax.named_scope("w_sum"):
      for k in range(16):
        @pl.when(o != k)
        def _():
            sum_copy(k, k).wait_recv()

    total = pltpu.roll(sum_in[...].sum(axis=0), (128 - 4 * o) % 128, 1)[:1]
    fb_out[...] = total[:, :4]

    with jax.named_scope("w_send"):
      for k in range(16):
        @pl.when(o != k)
        def _():
            chunk_copy(k).wait_send()
            sum_copy(k, o).wait_send()

        @pl.when(w != k)
        def _():
            t_copy(k, w).wait_send()
            part_copy(k, w).wait_send()


def finish(total, shift, rotated, fb_out, rot_out, fb_v, sems):
    copies = [
        pltpu.make_async_copy(rotated.at[g], rot_out.at[g], sems.at[g]) for g in range(4)
    ]
    for copy in copies:
        copy.start()
    fb_v[...] = total[...] - shift[...]
    copies.append(pltpu.make_async_copy(fb_v, fb_out, sems.at[4]))
    copies[4].start()
    for copy in copies:
        copy.wait()


def local(chol, orbitals, greens, shift):
    anywhere = pl.BlockSpec(memory_space=pltpu.HBM)
    in_vmem = pl.BlockSpec(memory_space=pltpu.VMEM)
    sems = [pltpu.SemaphoreType.DMA((16,))] * 8
    force_bias, rotated = pl.pallas_call(
        kernel,
        out_shape=(
            jax.ShapeDtypeStruct((1, 4), F32),
            jax.ShapeDtypeStruct((4, 1024, 128), BF16),
        ),
        in_specs=[anywhere] * 3,
        out_specs=(in_vmem, in_vmem),
        scratch_shapes=[
            pltpu.VMEM((2, 128, 1024), BF16),
            pltpu.VMEM((8, 1024, 256), BF16),
            pltpu.VMEM((2048, 1024), BF16),
            pltpu.VMEM((1024, 2048), BF16),
            pltpu.VMEM((64, 128, 128), BF16),
            pltpu.VMEM((16, 4, 128, 128), BF16),
            pltpu.VMEM((1024, 512), F32),
            pltpu.VMEM((16, 128, 128), BF16),
            pltpu.VMEM((16, 128, 128), BF16),
            pltpu.VMEM((128, 64), F32),
            pltpu.VMEM((128, 256), F32),
            pltpu.VMEM((16, 8, 128), F32),
            pltpu.VMEM((16, 8, 128), F32),
            pltpu.VMEM((8, 128), F32),
            pltpu.VMEM((16, 8, 128), F32),
            pltpu.SemaphoreType.REGULAR,
            pltpu.SemaphoreType.REGULAR((2,)),
            pltpu.SemaphoreType.DMA((5,)),
            pltpu.SemaphoreType.DMA((8,)),
            *sems,
        ],
        compiler_params=pltpu.CompilerParams(
            collective_id=0, has_side_effects=True, vmem_limit_bytes=52 * 2**20
        ),
        name="half_rotation",
    )(chol, orbitals, greens)
    return pl.pallas_call(
        finish,
        out_shape=(
            jax.ShapeDtypeStruct((1, 4), F32),
            jax.ShapeDtypeStruct((4, 1024, 128), BF16),
        ),
        in_specs=[in_vmem] * 3,
        out_specs=(anywhere, anywhere),
        scratch_shapes=[pltpu.VMEM((1, 4), F32), pltpu.SemaphoreType.DMA((5,))],
        compiler_params=pltpu.CompilerParams(vmem_limit_bytes=2**20),
        name="finish",
    )(force_bias, shift.reshape(1, 4), rotated)


def solution(mesh):
    return jax.shard_map(
        local,
        mesh=mesh,
        in_specs=(P(None, "orb", "walk"), P(), P("walk", None, None), P("orb")),
        out_specs=(P("walk", "orb"), P("orb", None, "walk")),
        check_vma=False,
    )
```

```python
import jax
import jax.numpy as jnp
from jax import lax
from jax.experimental import pallas as pl
from jax.experimental.pallas import tpu as pltpu
from jax.sharding import PartitionSpec as P

MESH = pl.DeviceIdType.MESH
F32, BF16 = jnp.float32, jnp.bfloat16
FAR_FIRST = (4, 3, 5, 2, 6, 1, 7, 0)

def kernel(
    chol, orbitals, greens, fb_out, rot_out,
    rows_v, greens_v, orb_v, orb_t, chol_v, chunks, acc,
    t_out, t_in, diag_few, diag_all, part_out, part_in, sum_out, sum_in,
    orb_ready, walk_ready, load_sem, greens_sem,
    chol_send, chol_recv, t_send, t_recv, part_send, part_recv, sum_send, sum_recv,
):
    o, w = lax.axis_index("orb"), lax.axis_index("walk")
    y, a, c = o // 4, (o // 2) % 2, o % 2
    z, h = w // 2, w % 2
    across = y * 4 + (1 - a) * 2 + c
    pair = (o // 2) * 2
    partner = pair + 1 - c

    def place(orb, walk):
        return {"orb": orb, "walk": walk}

    def met(walk):
        return place(jnp.where(walk % 2 == h, o, across), walk)

    def signal(sem, where):
        pl.semaphore_signal(sem, inc=1, device_id=where, device_id_type=MESH)

    def await_some(sem, amount):
        @pl.when(amount > 0)
        def _():
            pl.semaphore_wait(sem, amount)

    def loop(start, stop, body):
        lax.fori_loop(start, stop, lambda i, _: body(i), None)

    es = jax.named_scope('e_sig'); es.__enter__()
    barrier = pltpu.get_barrier_semaphore()
    loop(8, jnp.where(z < 4, 16, 0), lambda i: signal(barrier, met(i)))
    signal(barrier, place(partner, w))
    loop(pair + 2, 16, lambda i: signal(barrier, place(i, w)))
    loop(w + 1, 8, lambda i: signal(barrier, met(i)))

    es.__exit__(None,None,None)
    es = jax.named_scope('e_load'); es.__enter__()
    own_rows = pltpu.make_async_copy(
        orbitals.at[pl.ds(pl.multiple_of(o * 128, 128), 128)], rows_v.at[h], load_sem.at[0]
    )
    far_rows = pltpu.make_async_copy(
        orbitals.at[pl.ds(pl.multiple_of(across * 128, 128), 128)], rows_v.at[1 - h], load_sem.at[1]
    )
    own_rows.start()
    far_rows.start()
    columns = []
    for k, dz in enumerate(FAR_FIRST):
        there = pl.multiple_of(((z + dz) % 8) * 256, 256)
        copy = pltpu.make_async_copy(
            greens.at[0, :, pl.ds(there, 256)], greens_v.at[k], greens_sem.at[k]
        )
        copy.start()
        columns.append(copy)
    es.__exit__(None,None,None)
    with jax.named_scope("w_bar"):
        pl.semaphore_wait(barrier, pair + 1 + jnp.minimum(w, 8))
    loop(0, jnp.minimum(w, 8), lambda i: signal(walk_ready.at[w // 8], met(i)))
    loop(0, pair, lambda i: signal(orb_ready, place(i, w)))

    def chunk_copy(to):
        return pltpu.make_async_remote_copy(
            src_ref=chol.at[pl.ds(4 * to, 4)],
            dst_ref=chunks.at[o],
            send_sem=chol_send.at[to],
            recv_sem=chol_recv.at[o],
            device_id=place(to, w),
            device_id_type=MESH,
        )

    def chunk_arrival(source):
        pltpu.make_async_remote_copy(
            src_ref=chol.at[pl.ds(4 * source, 4)],
            dst_ref=chunks.at[source],
            send_sem=chol_send.at[source],
            recv_sem=chol_recv.at[source],
            device_id=place(source, w),
            device_id_type=MESH,
        ).wait_recv()

    def chip(dy, da):
        return ((y + dy) % 4) * 2 + (a + da) % 2

    order = ((2, 1), (1, 1), (3, 1), (0, 1), (2, 0), (1, 0), (3, 0))

    def scatter_all():
        with jax.named_scope("w_orb"):
            await_some(orb_ready, 14 - pair)
        for dy, da in order:
            for dc in range(2):
                chunk_copy(chip(dy, da) * 2 + (c + dc) % 2).start()
        chunk_copy(partner).start()

    all_rows = pltpu.make_async_copy(orbitals, orb_v, load_sem.at[2])
    own_chol = pltpu.make_async_copy(chol, chol_v, load_sem.at[3])
    own_chunk = pltpu.make_async_copy(chol.at[pl.ds(4 * o, 4)], chunks.at[o], load_sem.at[4])

    def t_copy(to, source):
        return pltpu.make_async_remote_copy(
            src_ref=t_out.at[to],
            dst_ref=t_in.at[source],
            send_sem=t_send.at[to],
            recv_sem=t_recv.at[source],
            device_id=met(to),
            device_id_type=MESH,
        )

    def send_products(wanted):
        for dz in FAR_FIRST:
            for dh in (1, 0):
                to = ((z + dz) % 8) * 2 + (h + dh) % 2

                @pl.when(wanted(to))
                def _():
                    t_copy(to, w).start()

    own_rows.wait()
    far_rows.wait()

    def products(start, stop):
        for k in range(start, stop):
            columns[k].wait()
        for k in range(start, stop):
            there = (z + FAR_FIRST[k]) % 8
            both = jnp.dot(
                rows_v[...].reshape(256, 1024), greens_v[k], preferred_element_type=F32
            ).astype(BF16)
            t_out[2 * there] = both[:128, :128]
            t_out[2 * there + 1] = both[128:, 128:]

    def all_products():
        with jax.named_scope("prod1"):
            products(0, 4)
        all_rows.start()
        own_chol.start()
        own_chunk.start()
        with jax.named_scope("prod"):
            products(4, 8)

        @pl.when(z >= 4)
        def _():
            send_products(lambda to: to < 8)

    @pl.when(y < 2)
    def _():
        all_products()
        scatter_all()

    @pl.when(y >= 2)
    def _():
        scatter_all()
        all_products()

    def products_from(first, count):
        for k in range(first, first + count):

            @pl.when(w != k)
            def _():
                t_copy(k, k).wait_recv()

    patient = (z == 2) | (z == 3)
    with jax.named_scope("w_walk0"):
        await_some(walk_ready.at[0], 7 - w)

    @pl.when(z < 4)
    def _():
        send_products(lambda to: (to < 8) & (to != w))


    all_rows.wait()

    def turn(i):
        at = pl.ds(pl.multiple_of(i * 128, 128), 128)
        orb_t[:, at] = orb_v[at, :].T

    with jax.named_scope("turn"):
        loop(0, 16, turn)

    @pl.when(patient)
    def _():
        with jax.named_scope("w_pat"):
            products_from(0, 2)

    with jax.named_scope("w_walk1"):
        @pl.when(z < 4)
        def _():
            pl.semaphore_wait(walk_ready.at[1], 8)

        @pl.when(w == 7)
        def _():
            loop(8, 16, lambda i: signal(walk_ready.at[0], met(i)))

        @pl.when(z >= 4)
        def _():
            pl.semaphore_wait(walk_ready.at[0], 1)

    send_products(lambda to: (to >= 8) & (to != w))
    t_in[w] = t_out[w]

    def rotate(group, first=False, last=False):
        spots = []
        for dy, da in group:
            there = chip(dy, da)
            with jax.named_scope(f"w_c{dy}{da}"):
                if dy or da:
                    chunk_arrival(2 * there)
                    chunk_arrival(2 * there + 1)
                else:
                    own_chunk.wait()
                    chunk_arrival(partner)
            spots.append(there)
        with jax.named_scope(f"rot{group[0][0]}{group[0][1]}"):
            left = jnp.concatenate(
                [orb_t[:, pl.ds(pl.multiple_of(there * 256, 256), 256)] for there in spots], axis=1
            )
            for n in range(2):
                block = jnp.concatenate(
                    [
                        jnp.concatenate(
                            [chunks[2 * there + i, g] for there in spots for i in range(2)], axis=0
                        )
                        for g in (2 * n, 2 * n + 1)
                    ],
                    axis=1,
                )
                term = jnp.dot(left, block, preferred_element_type=F32)
                at = slice(256 * n, 256 * n + 256)
                if not first:
                    term = acc[:, at] + term
                if last:
                    rot_out[2 * n] = term[:, :128].astype(BF16)
                    rot_out[2 * n + 1] = term[:, 128:].astype(BF16)
                else:
                    acc[:, at] = term

    def part_copy(to, source):
        return pltpu.make_async_remote_copy(
            src_ref=part_out.at[to],
            dst_ref=part_in.at[source],
            send_sem=part_send.at[to],
            recv_sem=part_recv.at[source],
            device_id=met(to),
            device_id_type=MESH,
        )

    def terms(count, skipped, diag):
        lanes = 16 * count
        right = jnp.concatenate(
            [t_in[:count, 16 * b : 16 * b + 16, :].reshape(lanes, 128) for b in range(8)], axis=1
        )
        same_row = (
            lax.broadcasted_iota(jnp.int32, (256, lanes), 1) % 16
            == lax.broadcasted_iota(jnp.int32, (256, lanes), 0) % 16
        )
        for j in range(4):
            at = slice(16 * j, 16 * j + 16)
            left = jnp.concatenate(
                [chol_v[at, 16 * b : 16 * b + 16, :].reshape(256, 128) for b in range(8)],
                axis=1,
            )
            product = lax.dot_general(
                left, right, (((1,), (1,)), ((), ())), preferred_element_type=F32
            )
            diag[at, :] = jnp.where(same_row, product, 0.0).reshape(16, 16, lanes).sum(axis=1)

        picks = jnp.where(
            lax.broadcasted_iota(jnp.int32, (16, lanes), 1) // 16
            == lax.broadcasted_iota(jnp.int32, (16, lanes), 0),
            1.0, 0.0,
        )
        sums = lax.dot_general(
            picks, diag[...], (((1,), (1,)), ((), ())),
            precision=lax.Precision.HIGHEST, preferred_element_type=F32,
        )
        for k in range(skipped, count):
            part_out[k] = sums[k : k + 1, :]
        for k in range(skipped, count):

            @pl.when(w != k)
            def _():
                part_copy(k, w).start()

    diag_few[64:, :] = jnp.zeros((64, 64), F32)
    diag_all[64:, :] = jnp.zeros((64, 256), F32)
    rotate(((0, 0),), first=True)
    own_chol.wait()
    with jax.named_scope("w_t0"):

        @pl.when(jnp.logical_not(patient))
        def _():
            products_from(0, 2)

        products_from(2, 2)

    with jax.named_scope("terms0"):
        terms(4, 0, diag_few)
    with jax.named_scope("w_t4"):
        products_from(4, 12)
    with jax.named_scope("terms4"):
        terms(16, 4, diag_all)
    part_in[w] = part_out[w]
    with jax.named_scope("w_part"):
      for k in range(16):
        @pl.when(w != k)
        def _():
            part_copy(k, k).wait_recv()

    sum_out[...] = part_in[...].sum(axis=0)

    def sum_copy(to, source):
        return pltpu.make_async_remote_copy(
            src_ref=sum_out,
            dst_ref=sum_in.at[source],
            send_sem=sum_send.at[to],
            recv_sem=sum_recv.at[source],
            device_id=place(to, w),
            device_id_type=MESH,
        )

    for dy in (2, 1, 3, 0):
        for da in (1, 0):
            for dc in range(2):
                if dy or da or dc:
                    sum_copy(chip(dy, da) * 2 + (c + dc) % 2, o).start()
    sum_in[o] = sum_out[...]
    rotate(((2, 0), (2, 1)))
    rotate(((1, 1), (3, 1)))
    rotate(((1, 0), (3, 0), (0, 1)), last=True)
    with jax.named_scope("w_sum"):
      for k in range(16):
        @pl.when(o != k)
        def _():
            sum_copy(k, k).wait_recv()

    total = pltpu.roll(sum_in[...].sum(axis=0), (128 - 4 * o) % 128, 1)[:1]
    fb_out[...] = total[:, :4]

    with jax.named_scope("w_send"):
      for k in range(16):
        @pl.when(o != k)
        def _():
            chunk_copy(k).wait_send()
            sum_copy(k, o).wait_send()

        @pl.when(w != k)
        def _():
            t_copy(k, w).wait_send()
            part_copy(k, w).wait_send()


def finish(total, shift, rotated, fb_out, rot_out, fb_v, sems):
    copies = [
        pltpu.make_async_copy(rotated.at[g], rot_out.at[g], sems.at[g]) for g in range(4)
    ]
    for copy in copies:
        copy.start()
    fb_v[...] = total[...] - shift[...]
    copies.append(pltpu.make_async_copy(fb_v, fb_out, sems.at[4]))
    copies[4].start()
    for copy in copies:
        copy.wait()


def local(chol, orbitals, greens, shift):
    anywhere = pl.BlockSpec(memory_space=pltpu.HBM)
    in_vmem = pl.BlockSpec(memory_space=pltpu.VMEM)
    sems = [pltpu.SemaphoreType.DMA((16,))] * 8
    force_bias, rotated = pl.pallas_call(
        kernel,
        out_shape=(
            jax.ShapeDtypeStruct((1, 4), F32),
            jax.ShapeDtypeStruct((4, 1024, 128), BF16),
        ),
        in_specs=[anywhere] * 3,
        out_specs=(in_vmem, in_vmem),
        scratch_shapes=[
            pltpu.VMEM((2, 128, 1024), BF16),
            pltpu.VMEM((8, 1024, 256), BF16),
            pltpu.VMEM((2048, 1024), BF16),
            pltpu.VMEM((1024, 2048), BF16),
            pltpu.VMEM((64, 128, 128), BF16),
            pltpu.VMEM((16, 4, 128, 128), BF16),
            pltpu.VMEM((1024, 512), F32),
            pltpu.VMEM((16, 128, 128), BF16),
            pltpu.VMEM((16, 128, 128), BF16),
            pltpu.VMEM((128, 64), F32),
            pltpu.VMEM((128, 256), F32),
            pltpu.VMEM((16, 1, 128), F32),
            pltpu.VMEM((16, 1, 128), F32),
            pltpu.VMEM((1, 128), F32),
            pltpu.VMEM((16, 1, 128), F32),
            pltpu.SemaphoreType.REGULAR,
            pltpu.SemaphoreType.REGULAR((2,)),
            pltpu.SemaphoreType.DMA((5,)),
            pltpu.SemaphoreType.DMA((8,)),
            *sems,
        ],
        compiler_params=pltpu.CompilerParams(
            collective_id=0, has_side_effects=True, vmem_limit_bytes=52 * 2**20
        ),
        name="half_rotation",
    )(chol, orbitals, greens)
    return pl.pallas_call(
        finish,
        out_shape=(
            jax.ShapeDtypeStruct((1, 4), F32),
            jax.ShapeDtypeStruct((4, 1024, 128), BF16),
        ),
        in_specs=[in_vmem] * 3,
        out_specs=(anywhere, anywhere),
        scratch_shapes=[pltpu.VMEM((1, 4), F32), pltpu.SemaphoreType.DMA((5,))],
        compiler_params=pltpu.CompilerParams(vmem_limit_bytes=2**20),
        name="finish",
    )(force_bias, shift.reshape(1, 4), rotated)


def solution(mesh):
    return jax.shard_map(
        local,
        mesh=mesh,
        in_specs=(P(None, "orb", "walk"), P(), P("walk", None, None), P("orb")),
        out_specs=(P("walk", "orb"), P("orb", None, "walk")),
        check_vma=False,
    )
```

```python
import jax
import jax.numpy as jnp
from jax import lax
from jax.experimental import pallas as pl
from jax.experimental.pallas import tpu as pltpu
from jax.sharding import PartitionSpec as P

MESH = pl.DeviceIdType.MESH
F32, BF16 = jnp.float32, jnp.bfloat16
FAR_FIRST = (4, 3, 5, 2, 6, 1, 7, 0)

def kernel(
    chol, orbitals, greens, fb_out, rot_out,
    rows_v, greens_v, orb_v, orb_t, chol_v, chunks, acc,
    t_out, t_in, diag_few, diag_all, part_out, part_in, sum_out, sum_in,
    orb_ready, walk_ready, load_sem, greens_sem,
    chol_send, chol_recv, t_send, t_recv, part_send, part_recv, sum_send, sum_recv,
):
    o, w = lax.axis_index("orb"), lax.axis_index("walk")
    y, a, c = o // 4, (o // 2) % 2, o % 2
    z, h = w // 2, w % 2
    across = y * 4 + (1 - a) * 2 + c
    pair = (o // 2) * 2
    partner = pair + 1 - c

    def place(orb, walk):
        return {"orb": orb, "walk": walk}

    def met(walk):
        return place(jnp.where(walk % 2 == h, o, across), walk)

    def signal(sem, where):
        pl.semaphore_signal(sem, inc=1, device_id=where, device_id_type=MESH)

    def await_some(sem, amount):
        @pl.when(amount > 0)
        def _():
            pl.semaphore_wait(sem, amount)

    def loop(start, stop, body):
        lax.fori_loop(start, stop, lambda i, _: body(i), None)

    es = jax.named_scope('e_sig'); es.__enter__()
    barrier = pltpu.get_barrier_semaphore()
    loop(8, jnp.where(z < 4, 16, 0), lambda i: signal(barrier, met(i)))
    signal(barrier, place(partner, w))
    loop(pair + 2, 16, lambda i: signal(barrier, place(i, w)))
    loop(w + 1, 8, lambda i: signal(barrier, met(i)))

    es.__exit__(None,None,None)
    es = jax.named_scope('e_load'); es.__enter__()
    own_rows = pltpu.make_async_copy(
        orbitals.at[pl.ds(pl.multiple_of(o * 128, 128), 128)], rows_v.at[h], load_sem.at[0]
    )
    far_rows = pltpu.make_async_copy(
        orbitals.at[pl.ds(pl.multiple_of(across * 128, 128), 128)], rows_v.at[1 - h], load_sem.at[1]
    )
    own_rows.start()
    far_rows.start()
    columns = []
    for k, dz in enumerate(FAR_FIRST):
        there = pl.multiple_of(((z + dz) % 8) * 256, 256)
        copy = pltpu.make_async_copy(
            greens.at[0, :, pl.ds(there, 256)], greens_v.at[k], greens_sem.at[k]
        )
        copy.start()
        columns.append(copy)
    es.__exit__(None,None,None)
    with jax.named_scope("w_bar"):
        pl.semaphore_wait(barrier, pair + 1 + jnp.minimum(w, 8))
    loop(0, jnp.minimum(w, 8), lambda i: signal(walk_ready.at[w // 8], met(i)))
    loop(0, pair, lambda i: signal(orb_ready, place(i, w)))

    def chunk_copy(to):
        return pltpu.make_async_remote_copy(
            src_ref=chol.at[pl.ds(4 * to, 4)],
            dst_ref=chunks.at[o],
            send_sem=chol_send.at[to],
            recv_sem=chol_recv.at[o],
            device_id=place(to, w),
            device_id_type=MESH,
        )

    def chunk_arrival(source):
        pltpu.make_async_remote_copy(
            src_ref=chol.at[pl.ds(4 * source, 4)],
            dst_ref=chunks.at[source],
            send_sem=chol_send.at[source],
            recv_sem=chol_recv.at[source],
            device_id=place(source, w),
            device_id_type=MESH,
        ).wait_recv()

    def chip(dy, da):
        return ((y + dy) % 4) * 2 + (a + da) % 2

    order = ((2, 1), (1, 1), (3, 1), (0, 1), (2, 0), (1, 0), (3, 0))

    def scatter_all():
        with jax.named_scope("w_orb"):
            await_some(orb_ready, 14 - pair)
        for dy, da in order:
            for dc in range(2):
                chunk_copy(chip(dy, da) * 2 + (c + dc) % 2).start()
        chunk_copy(partner).start()

    all_rows = pltpu.make_async_copy(orbitals, orb_v, load_sem.at[2])
    own_chol = pltpu.make_async_copy(chol, chol_v, load_sem.at[3])
    own_chunk = pltpu.make_async_copy(chol.at[pl.ds(4 * o, 4)], chunks.at[o], load_sem.at[4])

    def t_copy(to, source):
        return pltpu.make_async_remote_copy(
            src_ref=t_out.at[to],
            dst_ref=t_in.at[source],
            send_sem=t_send.at[to],
            recv_sem=t_recv.at[source],
            device_id=met(to),
            device_id_type=MESH,
        )

    def send_products(wanted):
        for dz in FAR_FIRST:
            for dh in (1, 0):
                to = ((z + dz) % 8) * 2 + (h + dh) % 2

                @pl.when(wanted(to))
                def _():
                    t_copy(to, w).start()

    own_rows.wait()
    far_rows.wait()

    def products(start, stop):
        for k in range(start, stop):
            columns[k].wait()
        for k in range(start, stop):
            there = (z + FAR_FIRST[k]) % 8
            both = jnp.dot(
                rows_v[...].reshape(256, 1024), greens_v[k], preferred_element_type=F32
            ).astype(BF16)
            t_out[2 * there] = both[:128, :128]
            t_out[2 * there + 1] = both[128:, 128:]

    def all_products():
        with jax.named_scope("prod1"):
            products(0, 4)
        all_rows.start()
        own_chol.start()
        own_chunk.start()
        with jax.named_scope("prod"):
            products(4, 8)

        @pl.when(z >= 4)
        def _():
            send_products(lambda to: to < 8)

    @pl.when(y < 2)
    def _():
        all_products()
        scatter_all()

    @pl.when(y >= 2)
    def _():
        scatter_all()
        all_products()

    def products_from(first, count):
        for k in range(first, first + count):

            @pl.when(w != k)
            def _():
                t_copy(k, k).wait_recv()

    patient = (z == 2) | (z == 3)
    with jax.named_scope("w_walk0"):
        await_some(walk_ready.at[0], 7 - w)

    @pl.when(z < 4)
    def _():
        send_products(lambda to: (to < 8) & (to != w))


    all_rows.wait()

    def turn(i):
        at = pl.ds(pl.multiple_of(i * 128, 128), 128)
        orb_t[:, at] = orb_v[at, :].T

    with jax.named_scope("turn"):
        loop(0, 16, turn)

    @pl.when(patient)
    def _():
        with jax.named_scope("w_pat"):
            products_from(0, 2)

    with jax.named_scope("w_walk1"):
        @pl.when(z < 4)
        def _():
            pl.semaphore_wait(walk_ready.at[1], 8)

        @pl.when(w == 7)
        def _():
            loop(8, 16, lambda i: signal(walk_ready.at[0], met(i)))

        @pl.when(z >= 4)
        def _():
            pl.semaphore_wait(walk_ready.at[0], 1)

    send_products(lambda to: (to >= 8) & (to != w))
    t_in[w] = t_out[w]

    def rotate(group, first=False, last=False):
        spots = []
        for dy, da in group:
            there = chip(dy, da)
            with jax.named_scope(f"w_c{dy}{da}"):
                if dy or da:
                    chunk_arrival(2 * there)
                    chunk_arrival(2 * there + 1)
                else:
                    own_chunk.wait()
                    chunk_arrival(partner)
            spots.append(there)
        with jax.named_scope(f"rot{group[0][0]}{group[0][1]}"):
            left = jnp.concatenate(
                [orb_t[:, pl.ds(pl.multiple_of(there * 256, 256), 256)] for there in spots], axis=1
            )
            for n in range(2):
                block = jnp.concatenate(
                    [
                        jnp.concatenate(
                            [chunks[2 * there + i, g] for there in spots for i in range(2)], axis=0
                        )
                        for g in (2 * n, 2 * n + 1)
                    ],
                    axis=1,
                )
                term = jnp.dot(left, block, preferred_element_type=F32)
                at = slice(256 * n, 256 * n + 256)
                if not first:
                    term = acc[:, at] + term
                if last:
                    rot_out[2 * n] = term[:, :128].astype(BF16)
                    rot_out[2 * n + 1] = term[:, 128:].astype(BF16)
                else:
                    acc[:, at] = term

    def part_copy(to, source):
        return pltpu.make_async_remote_copy(
            src_ref=part_out.at[to],
            dst_ref=part_in.at[source],
            send_sem=part_send.at[to],
            recv_sem=part_recv.at[source],
            device_id=met(to),
            device_id_type=MESH,
        )

    def terms(count, skipped, diag):
        lanes = 16 * count
        right = jnp.concatenate(
            [t_in[:count, 16 * b : 16 * b + 16, :].reshape(lanes, 128) for b in range(8)], axis=1
        )
        same_row = (
            lax.broadcasted_iota(jnp.int32, (256, lanes), 1) % 16
            == lax.broadcasted_iota(jnp.int32, (256, lanes), 0) % 16
        )
        for j in range(4):
            at = slice(16 * j, 16 * j + 16)
            left = jnp.concatenate(
                [chol_v[at, 16 * b : 16 * b + 16, :].reshape(256, 128) for b in range(8)],
                axis=1,
            )
            product = lax.dot_general(
                left, right, (((1,), (1,)), ((), ())), preferred_element_type=F32
            )
            diag[at, :] = jnp.where(same_row, product, 0.0).reshape(16, 16, lanes).sum(axis=1)

        picks = jnp.where(
            lax.broadcasted_iota(jnp.int32, (16, lanes), 1) // 16
            == lax.broadcasted_iota(jnp.int32, (16, lanes), 0),
            1.0, 0.0,
        )
        sums = lax.dot_general(
            picks, diag[...], (((1,), (1,)), ((), ())),
            precision=lax.Precision.HIGHEST, preferred_element_type=F32,
        )
        for k in range(skipped, count):
            part_out[k] = sums[k : k + 1, :]
        for k in range(skipped, count):

            @pl.when(w != k)
            def _():
                part_copy(k, w).start()

    diag_few[64:, :] = jnp.zeros((64, 64), F32)
    diag_all[64:, :] = jnp.zeros((64, 256), F32)
    rotate(((0, 0),), first=True)
    own_chol.wait()
    with jax.named_scope("w_t0"):

        @pl.when(jnp.logical_not(patient))
        def _():
            products_from(0, 2)

        products_from(2, 2)

    with jax.named_scope("terms0"):
        terms(4, 0, diag_few)
    with jax.named_scope("w_t4"):
        products_from(4, 12)
    with jax.named_scope("terms4"):
        terms(16, 4, diag_all)
    part_in[w] = part_out[w]
    with jax.named_scope("w_part"):
      for k in range(16):
        @pl.when(w != k)
        def _():
            part_copy(k, k).wait_recv()

    sum_out[...] = part_in[...].sum(axis=0)

    def sum_copy(to, source):
        return pltpu.make_async_remote_copy(
            src_ref=sum_out,
            dst_ref=sum_in.at[source],
            send_sem=sum_send.at[to],
            recv_sem=sum_recv.at[source],
            device_id=place(to, w),
            device_id_type=MESH,
        )

    for dy in (2, 1, 3, 0):
        for da in (1, 0):
            for dc in range(2):
                if dy or da or dc:
                    sum_copy(chip(dy, da) * 2 + (c + dc) % 2, o).start()
    sum_in[o] = sum_out[...]
    rotate(((2, 0), (2, 1)))
    rotate(((1, 1), (3, 1)))
    rotate(((1, 0), (3, 0), (0, 1)), last=True)
    with jax.named_scope("w_send"):
      for k in range(16):
        @pl.when(o != k)
        def _():
            chunk_copy(k).wait_send()
            sum_copy(k, o).wait_send()

        @pl.when(w != k)
        def _():
            t_copy(k, w).wait_send()
            part_copy(k, w).wait_send()

    with jax.named_scope("w_sum"):
      for k in range(16):
        @pl.when(o != k)
        def _():
            sum_copy(k, k).wait_recv()

    total = pltpu.roll(sum_in[...].sum(axis=0), (128 - 4 * o) % 128, 1)[:1]
    fb_out[...] = total[:, :4]


def finish(total, shift, rotated, fb_out, rot_out, fb_v, sems):
    copies = [
        pltpu.make_async_copy(rotated.at[g], rot_out.at[g], sems.at[g]) for g in range(4)
    ]
    for copy in copies:
        copy.start()
    fb_v[...] = total[...] - shift[...]
    copies.append(pltpu.make_async_copy(fb_v, fb_out, sems.at[4]))
    copies[4].start()
    for copy in copies:
        copy.wait()


def local(chol, orbitals, greens, shift):
    anywhere = pl.BlockSpec(memory_space=pltpu.HBM)
    in_vmem = pl.BlockSpec(memory_space=pltpu.VMEM)
    sems = [pltpu.SemaphoreType.DMA((16,))] * 8
    force_bias, rotated = pl.pallas_call(
        kernel,
        out_shape=(
            jax.ShapeDtypeStruct((1, 4), F32),
            jax.ShapeDtypeStruct((4, 1024, 128), BF16),
        ),
        in_specs=[anywhere] * 3,
        out_specs=(in_vmem, in_vmem),
        scratch_shapes=[
            pltpu.VMEM((2, 128, 1024), BF16),
            pltpu.VMEM((8, 1024, 256), BF16),
            pltpu.VMEM((2048, 1024), BF16),
            pltpu.VMEM((1024, 2048), BF16),
            pltpu.VMEM((64, 128, 128), BF16),
            pltpu.VMEM((16, 4, 128, 128), BF16),
            pltpu.VMEM((1024, 512), F32),
            pltpu.VMEM((16, 128, 128), BF16),
            pltpu.VMEM((16, 128, 128), BF16),
            pltpu.VMEM((128, 64), F32),
            pltpu.VMEM((128, 256), F32),
            pltpu.VMEM((16, 1, 128), F32),
            pltpu.VMEM((16, 1, 128), F32),
            pltpu.VMEM((1, 128), F32),
            pltpu.VMEM((16, 1, 128), F32),
            pltpu.SemaphoreType.REGULAR,
            pltpu.SemaphoreType.REGULAR((2,)),
            pltpu.SemaphoreType.DMA((5,)),
            pltpu.SemaphoreType.DMA((8,)),
            *sems,
        ],
        compiler_params=pltpu.CompilerParams(
            collective_id=0, has_side_effects=True, vmem_limit_bytes=52 * 2**20
        ),
        name="half_rotation",
    )(chol, orbitals, greens)
    return pl.pallas_call(
        finish,
        out_shape=(
            jax.ShapeDtypeStruct((1, 4), F32),
            jax.ShapeDtypeStruct((4, 1024, 128), BF16),
        ),
        in_specs=[in_vmem] * 3,
        out_specs=(anywhere, anywhere),
        scratch_shapes=[pltpu.VMEM((1, 4), F32), pltpu.SemaphoreType.DMA((5,))],
        compiler_params=pltpu.CompilerParams(vmem_limit_bytes=2**20),
        name="finish",
    )(force_bias, shift.reshape(1, 4), rotated)


def solution(mesh):
    return jax.shard_map(
        local,
        mesh=mesh,
        in_specs=(P(None, "orb", "walk"), P(), P("walk", None, None), P("orb")),
        out_specs=(P("walk", "orb"), P("orb", None, "walk")),
        check_vma=False,
    )
```
